512 devices in a mesh: users: 32 (over x, z_hi, core), hist: 16 (over y, z_lo).
Axes of the slice: x: 4, y: 8, z: 8 (z_hi: 4, z_lo: 2; z = z_hi * 2 + z_lo), core: 2. Of those that a mesh axis runs over, the one named last changes fastest.
Arguments:
- cand_x: bfloat16 [32768, 512], P(('users', 'hist')), parts along dimension 0, may hold values from -6 to 6
- hist_keys: bfloat16 [262144, 512], P(('users', 'hist')), parts along dimension 0, may hold values from -6 to 6
- hist_values: bfloat16 [262144, 512], P(('users', 'hist')), parts along dimension 0, may hold values from -6 to 6
- key_scale: bfloat16 [262144], P(('users', 'hist')), parts along dimension 0, may hold values from 0.5 to 2
- hist_len: int32 [32], P('users'), parts along dimension 0, may hold values from 2048 to 8192
- cand_limit: int32 [32768], P('users'), parts along dimension 0, may hold values from 1 to 8192
- ln_gain: float32 [512], replicated, may hold values from 0.1 to 1.9
- w_qu: bfloat16 [512, 1024], replicated, may hold values from -0.25 to 0.25
- w_out: bfloat16 [512, 512], replicated, may hold values from -0.25 to 0.25
Outputs:
- scored: bfloat16 [32768, 512], P(('users', 'hist')), parts along dimension 0
The draws below stay inside these ranges and needn't reach their ends.
There are 32 independent parts, one for each index of `users`. The reference program is written for one: setup_inputs(seed, part) draws one part's arguments, and reference() takes and returns one part's arrays. A program takes and returns all parts, laid end to end along the dimension named above; an argument that names none is the same for every part. Nothing has to cross between parts.
All inputs are finite; a program needn't handle non-finite values.
Results may differ from the reference program's by a relative error of at most 0.0058.
Values may be sent and summed in bfloat16 or wider, within the bound.
No kernel may reach another device: no remote copies, remote signals or barrier semaphores. Data moves between devices by JAX's collectives and lax.ppermute only.
A program may use at most 64 MiB of HBM per device.

```python
import math
import jax
import jax.numpy as jnp
from jax import lax

D = 512
HEADS = 8
CAND_DEV = 64
NC = 1024
HIST = 8192


def touch_ends(result, stream_key, low, largest):
    shape = result.shape
    index_at = [jax.random.randint(jax.random.fold_in(stream_key, axis), (), 0, shape[axis]) for axis in range(len(shape))]
    result = result.at[tuple(index_at)].set(low)
    longest = shape.index(max(shape))
    index_at[longest] = (index_at[longest] + 1) % shape[longest]
    return result.at[tuple(index_at)].set(largest)


def levels(rng, shape, pieces, smallest, top_value):
    factor_of = 1.0
    for position, shards_of in pieces:
        heights = jax.random.uniform(jax.random.fold_in(jax.random.fold_in(rng, 6), position), (shards_of,), jnp.float32, smallest / len(pieces), top_value / len(pieces))
        factor_of = factor_of * jnp.repeat(jnp.exp(heights), shape[position] // shards_of).reshape((-1,) + (1,) * (len(shape) - 1 - position))
    return factor_of


def noise(rng, extent, deviation, reach, pieces=(), held_as=jnp.bfloat16):
    level = levels(rng, extent, pieces, -0.22, 0.18) if pieces else 1.0
    array = jax.random.normal(rng, extent, jnp.float32) * deviation * level
    return jnp.minimum(jnp.maximum(array, -reach), reach).astype(held_as)


def setup_inputs(seed: int = 0, part: int = 0) -> dict:
    arg_keys = jax.random.split(jax.random.key(seed), 10)
    part_splits = jax.random.split(jax.random.fold_in(arg_keys[9], part), 10)
    cand_x = noise(part_splits[0], (NC, D), 1.0, 6.0, ((0, 16),))
    hist_keys = noise(part_splits[1], (HIST, D), 1.0, 6.0, ((0, 16),))
    hist_values = noise(part_splits[2], (HIST, D), 1.0, 6.0, ((0, 16),))
    key_scale = jnp.clip(jnp.exp(math.log(2.0) - 1.3862944 * jax.random.uniform(part_splits[3], (HIST,), jnp.float32) ** levels(part_splits[3], (HIST,), ((0, 16),), -0.2, 0.2)), 0.5, 2.0).astype(jnp.bfloat16)
    hist_len = jax.random.randint(part_splits[4], (1,), HIST // 4, HIST + 1).astype(jnp.int32)
    cand_limit = touch_ends(jax.random.randint(part_splits[5], (NC,), 1, HIST + 1), jax.random.fold_in(part_splits[5], 1), 1, HIST).astype(jnp.int32)
    ln_gain = jnp.clip(1.0 + 0.18 * jax.random.normal(arg_keys[6], (D,), jnp.float32), 0.1, 1.9)
    w_qu = noise(arg_keys[7], (D, 2 * D), D ** -0.5, 0.25)
    w_out = noise(arg_keys[8], (D, D), D ** -0.5, 0.25)
    return dict(cand_x=cand_x, hist_keys=hist_keys, hist_values=hist_values, key_scale=key_scale, hist_len=hist_len, cand_limit=cand_limit, ln_gain=ln_gain, w_qu=w_qu, w_out=w_out)


def row_norm(values):
    center = lax.optimization_barrier(jnp.mean(values, axis=-1, keepdims=True))
    spread = lax.optimization_barrier(jnp.mean((values - center) ** 2, axis=-1, keepdims=True))
    return (values - center) / jnp.sqrt(spread + 1e-05)

def attend(query_rows, history_limits, key_rows, value_rows, scale_rows, offset_pos):
    count = query_rows.shape[0]
    length = key_rows.shape[0]
    width = query_rows.shape[1]
    head_size = width // HEADS
    query_head_blocks = query_rows.reshape(count, HEADS, head_size)
    key_head_blocks = key_rows.reshape(length, HEADS, head_size)
    value_head_blocks = value_rows.reshape(length, HEADS, head_size)
    attention_scores = jnp.einsum('ufe,yfe->fuy', query_head_blocks, key_head_blocks, preferred_element_type=jnp.float32)
    factor = scale_rows.astype(jnp.float32) / jnp.sqrt(jnp.float32(head_size))
    attention_scores = attention_scores * factor[None, None, :]
    positions = offset_pos + jnp.arange(length, dtype=jnp.int32)
    visible = positions[None, :] < history_limits[:, None]
    weight_matrices = jnp.where(visible[None], jax.nn.silu(attention_scores), 0.0).astype(jnp.bfloat16)
    summed_output = jnp.einsum('apn,naf->paf', weight_matrices, value_head_blocks, preferred_element_type=jnp.float32)
    return summed_output.reshape(count, width)

def reference(cand_x, hist_keys, hist_values, key_scale, hist_len, cand_limit, ln_gain, w_qu, w_out):
    inputs32 = cand_x.astype(jnp.float32)
    normed = (row_norm(inputs32) * ln_gain).astype(jnp.bfloat16)
    projected = jax.nn.silu(jnp.dot(normed, w_qu, preferred_element_type=jnp.float32))
    query_vectors = projected[:, :D].astype(jnp.bfloat16)
    gating = projected[:, D:]
    history_limits = jnp.minimum(cand_limit, hist_len[0]).astype(jnp.int32)
    blocks = NC // CAND_DEV

    def one_block(couple):
        return attend(couple[0], couple[1], hist_keys, hist_values, key_scale, jnp.int32(0))
    attended = lax.map(one_block, (query_vectors.reshape(blocks, CAND_DEV, D), history_limits.reshape(blocks, CAND_DEV)))
    attended = attended.reshape(NC, D)
    mixed = (row_norm(attended) * gating).astype(jnp.bfloat16)
    return (inputs32 + jnp.dot(mixed, w_out, preferred_element_type=jnp.float32)).astype(jnp.bfloat16)
```

```python
import jax
import jax.numpy as jnp
from jax import lax
from jax.experimental import pallas as pl
from jax.experimental.pallas import tpu as pltpu
from jax.sharding import Mesh, PartitionSpec as P


F32 = jnp.float32
BF16 = jnp.bfloat16
VM = pl.BlockSpec(memory_space=pltpu.VMEM)
SM = pl.BlockSpec(memory_space=pltpu.SMEM)
PARAMS = pltpu.CompilerParams(vmem_limit_bytes=40 * 1024 * 1024)


def center(v):
    mean = jnp.mean(v, axis=-1, keepdims=True)
    var = jnp.mean((v - mean) ** 2, axis=-1, keepdims=True)
    return (v - mean) / jnp.sqrt(var + 1e-5)


def project_kernel(x_ref, gain_ref, w_ref, q_ref, gate_ref):
    normed = (center(x_ref[...].astype(F32)) * gain_ref[...]).astype(BF16)
    p = jnp.dot(normed, w_ref[...], preferred_element_type=F32)
    p = p / (1.0 + jnp.exp(-p))
    width = p.shape[1] // 2
    q = p[:, :width].astype(BF16)
    for i in range(q_ref.shape[0]):
        q_ref[i] = q
    gate_ref[...] = p[:, width:]


def scale_kernel(k_ref, s_ref, o_ref):
    rows = k_ref.shape[0]
    col = jnp.broadcast_to(s_ref[...].astype(F32) * (1.0 / 16.0), (8, rows)).T[:, :1]
    o_ref[...] = (k_ref[...].astype(F32) * col).astype(BF16)


def attend_kernel(off_ref, q_ref, k0_ref, v0_ref, k1_ref, v1_ref, lim_ref, o_ref):
    rows = q_ref.shape[0]
    n = k0_ref.shape[0]
    R = 256
    lane = lax.broadcasted_iota(jnp.int32, (1, 128), 1)
    low = lane < 64
    for r in range(rows // R):
        rs = slice(r * R, (r + 1) * R)
        masks = []
        for s in range(2):
            pos = lax.broadcasted_iota(jnp.int32, (R, n), 1) + off_ref[s]
            masks.append(jnp.where(pos < lim_ref[rs], 1.0, 0.0).astype(BF16))
        for pair in range(q_ref.shape[1] // 128):
            cs = slice(pair * 128, (pair + 1) * 128)
            q = q_ref[rs, cs]
            acc = jnp.zeros((R, 128), F32)
            for s, (kr, vr) in enumerate(((k0_ref, v0_ref), (k1_ref, v1_ref))):
                k = kr[:, cs]
                v = vr[:, cs]
                for sel in (low, jnp.logical_not(low)):
                    qh = jnp.where(sel, q, jnp.zeros_like(q))
                    vh = jnp.where(sel, v, jnp.zeros_like(v))
                    u = lax.dot_general(qh, k, (((1,), (1,)), ((), ())), preferred_element_type=F32)
                    w = (u * (1.0 + jnp.tanh(u))).astype(BF16) * masks[s]
                    acc += jnp.dot(w, vh, preferred_element_type=F32)
            o_ref[rs, cs] = acc.astype(BF16)


def finish_kernel(t_ref, gate_ref, x_ref, w_ref, o_ref):
    total = jnp.sum(t_ref[...].astype(F32), axis=0)
    mixed = (center(total) * gate_ref[...]).astype(BF16)
    o_ref[...] = (x_ref[...].astype(F32) + jnp.dot(mixed, w_ref[...], preferred_element_type=F32)).astype(BF16)


def sds(shape, dtype=BF16):
    return jax.ShapeDtypeStruct(shape, dtype)


def layer(cand_x, hist_keys, hist_values, key_scale, hist_len, cand_limit, ln_gain, w_qu, w_out):
    own, width = cand_x.shape
    n = hist_keys.shape[0]
    ny = lax.axis_size("y")
    nz = lax.axis_size("z")
    y = lax.axis_index("y")
    z = lax.axis_index("z")
    swap = [(i, 1 - i) for i in range(nz)]

    def exchange(t):
        return lax.all_to_all(t.reshape(ny, own, width), "y", 0, 0, tiled=True)

    def swapped(t):
        return lax.ppermute(t, "z", swap)

    v_far = swapped(hist_values)
    q, gate = pl.pallas_call(
        project_kernel,
        out_shape=(sds((ny, own, width)), sds((own, width), F32)),
        in_specs=[VM] * 3, out_specs=(VM,) * 2, compiler_params=PARAMS, name="project",
    )(cand_x, ln_gain.reshape(1, width), w_qu)
    every_q = exchange(q).reshape(ny * own, width)
    k_own = pl.pallas_call(
        scale_kernel, out_shape=sds((n, width)), in_specs=[VM] * 2, out_specs=VM,
        compiler_params=PARAMS, name="scale",
    )(hist_keys, key_scale.reshape(1, n))
    k_far = swapped(k_own)

    limits = jnp.minimum(cand_limit, hist_len[0]).reshape(ny, nz, own)
    limits = lax.dynamic_index_in_dim(limits, z, 1, keepdims=False).reshape(ny * own, 1)
    offsets = jnp.stack([(y * nz + z) * n, (y * nz + 1 - z) * n]).astype(jnp.int32)

    outs = pl.pallas_call(
        attend_kernel, out_shape=sds((ny * own, width)), in_specs=[SM] + [VM] * 6, out_specs=VM,
        compiler_params=PARAMS, name="attend",
    )(offsets, every_q, k_own, hist_values, k_far, v_far, limits)
    totals = exchange(outs)
    return pl.pallas_call(
        finish_kernel, out_shape=sds((own, width)), in_specs=[VM] * 4, out_specs=VM,
        compiler_params=PARAMS, name="finish",
    )(totals, gate, cand_x, w_out)


def solution(mesh):
    users, hist = mesh.devices.shape
    grid = Mesh(mesh.devices.reshape(users, hist // 2, 2), ("users", "y", "z"))
    both = ("users", "y", "z")
    in_specs = (P(both, None), P(both, None), P(both, None), P(both), P("users"), P("users"), P(), P(), P())
    return jax.shard_map(
        layer, mesh=grid, in_specs=in_specs, out_specs=P(both, None), check_vma=False
    )
```

```python
import jax
import jax.numpy as jnp
from jax import lax
from jax.experimental import pallas as pl
from jax.experimental.pallas import tpu as pltpu
from jax.sharding import Mesh, PartitionSpec as P


F32 = jnp.float32
BF16 = jnp.bfloat16
VM = pl.BlockSpec(memory_space=pltpu.VMEM)
HB = pl.BlockSpec(memory_space=pltpu.HBM)
SM = pl.BlockSpec(memory_space=pltpu.SMEM)
PARAMS = pltpu.CompilerParams(vmem_limit_bytes=40 * 1024 * 1024)


def center(v):
    mean = jnp.mean(v, axis=-1, keepdims=True)
    var = jnp.mean((v - mean) ** 2, axis=-1, keepdims=True)
    return (v - mean) / jnp.sqrt(var + 1e-5)


def project_kernel(x_hbm, gain_hbm, w_hbm, q_ref, x_ref, gain_ref, w_ref, sems):
    width = w_ref.shape[1]
    loads = [
        pltpu.make_async_copy(x_hbm, x_ref, sems.at[0]),
        pltpu.make_async_copy(gain_hbm, gain_ref, sems.at[1]),
        pltpu.make_async_copy(w_hbm.at[:, pl.ds(0, width)], w_ref, sems.at[2]),
    ]
    for load in loads:
        load.start()
    loads[0].wait()
    loads[1].wait()
    normed = (center(x_ref[...].astype(F32)) * gain_ref[...]).astype(BF16)
    loads[2].wait()
    p = jnp.dot(normed, w_ref[...], preferred_element_type=F32)
    q = (p / (1.0 + jnp.exp(-p))).astype(BF16)
    half = width // 2
    ny = q_ref.shape[1]
    for h in range(2):
        for i in range(ny):
            q_ref[h, i] = q[:, h * half:(h + 1) * half]


def gate_kernel(x_ref, gain_ref, w_ref, gate_ref):
    width = x_ref.shape[1]
    normed = (center(x_ref[...].astype(F32)) * gain_ref[...]).astype(BF16)
    p = jnp.dot(normed, w_ref[:, width:], preferred_element_type=F32)
    gate_ref[...] = p / (1.0 + jnp.exp(-p))


def pack_kernel(k_ref, v_ref, s_ref, o_ref):
    rows, width = k_ref.shape
    half = width // 2
    col = jnp.broadcast_to(s_ref[...].astype(F32) * (1.0 / 16.0), (8, rows)).T[:, :1]
    k = (k_ref[...].astype(F32) * col).astype(BF16)
    for h in range(2):
        o_ref[h, :rows] = k[:, h * half:(h + 1) * half]
        o_ref[h, rows:] = v_ref[:, h * half:(h + 1) * half]


def attend_part(q_ref, kv_ref, mask, cs):
    n = kv_ref.shape[0] // 2
    low = lax.broadcasted_iota(jnp.int32, (1, 128), 1) < 64
    q = q_ref[:, cs]
    k = kv_ref[:n, cs]
    v = kv_ref[n:, cs]
    weights = []
    values = []
    for sel in (low, jnp.logical_not(low)):
        head = jnp.where(sel, q, jnp.zeros_like(q))
        u = lax.dot_general(head, k, (((1,), (1,)), ((), ())), preferred_element_type=F32)
        weights.append((u * (1.0 + jnp.tanh(u))).astype(BF16) * mask)
        values.append(jnp.where(sel, v, jnp.zeros_like(v)))
    return jnp.dot(jnp.concatenate(weights, 1), jnp.concatenate(values, 0), preferred_element_type=F32)


def seen(off, lim_ref, n):
    pos = lax.broadcasted_iota(jnp.int32, (lim_ref.shape[0], n), 1) + off
    return jnp.where(pos < lim_ref[...], 1.0, 0.0).astype(BF16)


def near_kernel(off_ref, q_ref, kv_ref, lim_ref, o_ref):
    mask = seen(off_ref[0], lim_ref, kv_ref.shape[0] // 2)
    for pair in range(q_ref.shape[1] // 128):
        cs = slice(pair * 128, (pair + 1) * 128)
        o_ref[:, cs] = attend_part(q_ref, kv_ref, mask, cs)


def far_kernel(off_ref, q_ref, kv_ref, lim_ref, near_ref, o_ref):
    mask = seen(off_ref[1], lim_ref, kv_ref.shape[0] // 2)
    for pair in range(q_ref.shape[1] // 128):
        cs = slice(pair * 128, (pair + 1) * 128)
        o_ref[:, cs] = (near_ref[:, cs] + attend_part(q_ref, kv_ref, mask, cs)).astype(BF16)


def finish_kernel(t_ref, gate_ref, x_ref, w_ref, o_ref):
    sides = [jnp.sum(t_ref[h].astype(F32), axis=0) for h in range(2)]
    total = jnp.concatenate(sides, axis=1)
    mixed = (center(total) * gate_ref[...]).astype(BF16)
    o_ref[...] = (x_ref[...].astype(F32) + jnp.dot(mixed, w_ref[...], preferred_element_type=F32)).astype(BF16)


def sds(shape, dtype=BF16):
    return jax.ShapeDtypeStruct(shape, dtype)


def layer(cand_x, hist_keys, hist_values, key_scale, hist_len, cand_limit, ln_gain, w_qu, w_out):
    own, width = cand_x.shape
    n = hist_keys.shape[0]
    half = width // 2
    ny = lax.axis_size("y")
    nz = lax.axis_size("z")
    y = lax.axis_index("y")
    z = lax.axis_index("z")
    swap = [(i, 1 - i) for i in range(nz)]
    def exchange(t):
        return lax.all_to_all(t.reshape(nz * ny, own, half), ("z", "y"), 0, 0, tiled=True)

    gain = ln_gain.reshape(1, width)
    q = pl.pallas_call(
        project_kernel, out_shape=sds((nz, ny, own, half)), in_specs=[HB] * 3, out_specs=VM,
        scratch_shapes=[
            pltpu.VMEM((own, width), BF16), pltpu.VMEM((1, width), F32), pltpu.VMEM((width, width), BF16),
            pltpu.SemaphoreType.DMA((3,)),
        ],
        compiler_params=PARAMS, name="project",
    )(*(pltpu.with_memory_space_constraint(v, pltpu.HBM) for v in (cand_x, gain, w_qu)))
    gate = pl.pallas_call(
        gate_kernel, out_shape=sds((own, width), F32), in_specs=[VM] * 3, out_specs=VM,
        compiler_params=PARAMS, name="gate",
    )(cand_x, gain, w_qu)
    every_q = exchange(q).reshape(nz * ny * own, half)
    kv = pl.pallas_call(
        pack_kernel, out_shape=sds((nz, 2 * n, half)), in_specs=[VM] * 3, out_specs=VM,
        compiler_params=PARAMS, name="pack",
    )(hist_keys, hist_values, key_scale.reshape(1, n))
    kv_own = lax.dynamic_index_in_dim(kv, z, 0, keepdims=False)
    kv_out = lax.dynamic_index_in_dim(kv, 1 - z, 0, keepdims=False)
    kv_far = lax.ppermute(kv_out, "z", swap)

    limits = jnp.minimum(cand_limit, hist_len[0]).reshape(ny, nz, own)
    limits = jnp.swapaxes(limits, 0, 1).reshape(nz * ny * own, 1)
    offsets = jnp.stack([(y * nz + z) * n, (y * nz + 1 - z) * n]).astype(jnp.int32)

    near = pl.pallas_call(
        near_kernel, out_shape=sds((nz * ny * own, half), F32), in_specs=[SM] + [VM] * 3, out_specs=VM,
        compiler_params=PARAMS, name="near",
    )(offsets, every_q, kv_own, limits)
    outs = pl.pallas_call(
        far_kernel, out_shape=sds((nz * ny * own, half)), in_specs=[SM] + [VM] * 4, out_specs=VM,
        compiler_params=PARAMS, name="far",
    )(offsets, every_q, kv_far, limits, near)
    totals = exchange(outs).reshape(nz, ny, own, half)
    return pl.pallas_call(
        finish_kernel, out_shape=sds((own, width)), in_specs=[VM] * 4, out_specs=VM,
        compiler_params=PARAMS, name="finish",
    )(totals, gate, cand_x, w_out)


def solution(mesh):
    users, hist = mesh.devices.shape
    grid = Mesh(mesh.devices.reshape(users, hist // 2, 2), ("users", "y", "z"))
    both = ("users", "y", "z")
    in_specs = (P(both, None), P(both, None), P(both, None), P(both), P("users"), P("users"), P(), P(), P())
    return jax.shard_map(layer, mesh=grid, in_specs=in_specs, out_specs=P(both, None), check_vma=False)
```

```python
import jax
import jax.numpy as jnp
from jax import lax
from jax.experimental import pallas as pl
from jax.experimental.pallas import tpu as pltpu
from jax.sharding import Mesh, PartitionSpec as P


F32 = jnp.float32
BF16 = jnp.bfloat16
VM = pl.BlockSpec(memory_space=pltpu.VMEM)
HB = pl.BlockSpec(memory_space=pltpu.HBM)
SM = pl.BlockSpec(memory_space=pltpu.SMEM)
PARAMS = pltpu.CompilerParams(vmem_limit_bytes=40 * 1024 * 1024)


def center(v):
    mean = jnp.mean(v, axis=-1, keepdims=True)
    var = jnp.mean((v - mean) ** 2, axis=-1, keepdims=True)
    return (v - mean) / jnp.sqrt(var + 1e-5)


def project_kernel(x_hbm, gain_hbm, w_hbm, q_ref, x_ref, gain_ref, w_ref, sems):
    width = w_ref.shape[1]
    loads = [
        pltpu.make_async_copy(x_hbm, x_ref, sems.at[0]),
        pltpu.make_async_copy(gain_hbm, gain_ref, sems.at[1]),
        pltpu.make_async_copy(w_hbm.at[:, pl.ds(0, width)], w_ref, sems.at[2]),
    ]
    for load in loads:
        load.start()
    loads[0].wait()
    loads[1].wait()
    normed = (center(x_ref[...].astype(F32)) * gain_ref[...]).astype(BF16)
    loads[2].wait()
    p = jnp.dot(normed, w_ref[...], preferred_element_type=F32)
    q = (p / (1.0 + jnp.exp(-p))).astype(BF16)
    parts, copies, _, part = q_ref.shape
    for h in range(parts):
        for i in range(copies):
            q_ref[h, i] = q[:, h * part:(h + 1) * part]


def gate_kernel(x_ref, gain_ref, w_ref, gate_ref):
    width = x_ref.shape[1]
    normed = (center(x_ref[...].astype(F32)) * gain_ref[...]).astype(BF16)
    p = jnp.dot(normed, w_ref[:, width:], preferred_element_type=F32)
    gate_ref[...] = p / (1.0 + jnp.exp(-p))


def pack_kernel(part_ref, k_ref, v_ref, s_ref, *outs):
    rows, width = k_ref.shape
    part = width // len(outs)
    col = jnp.broadcast_to(s_ref[...].astype(F32).reshape(1, rows) * (1.0 / 16.0), (8, rows)).T[:, :1]
    k = (k_ref[...].astype(F32) * col).astype(BF16)
    for h in range(len(outs)):

        @pl.when(part_ref[0] == h)
        def _():
            for flip, out in enumerate(outs):
                cs = slice((h ^ flip) * part, ((h ^ flip) + 1) * part)
                out[:rows] = k[:, cs]
                out[rows:] = v_ref[:, cs]


def attend_pair(q, parts, cs):
    low = lax.broadcasted_iota(jnp.int32, (1, 128), 1) < 64
    weights = []
    values = []
    for kv_ref, mask in parts:
        n = kv_ref.shape[0] // 2
        k = kv_ref[:n, cs]
        v = kv_ref[n:, cs]
        for sel in (low, jnp.logical_not(low)):
            head = jnp.where(sel, q, jnp.zeros_like(q))
            u = lax.dot_general(head, k, (((1,), (1,)), ((), ())), preferred_element_type=F32)
            weights.append((u * (1.0 + jnp.tanh(u))).astype(BF16) * mask)
            values.append(jnp.where(sel, v, jnp.zeros_like(v)))
    return jnp.dot(jnp.concatenate(weights, 1), jnp.concatenate(values, 0), preferred_element_type=F32)


def seen(off, lim_ref, kv_ref):
    pos = lax.broadcasted_iota(jnp.int32, (lim_ref.shape[0], kv_ref.shape[0] // 2), 1) + off
    return jnp.where(pos < lim_ref[...], 1.0, 0.0).astype(BF16)


def near_kernel(off_ref, q_ref, own_ref, side_ref, lim_ref, o_ref):
    parts = [(ref, seen(off_ref[i], lim_ref, ref)) for i, ref in enumerate((own_ref, side_ref))]
    o_ref[...] = attend_pair(q_ref[...], parts, slice(None))


def far_kernel(off_ref, q_ref, side_ref, both_ref, lim_ref, near_ref, o_ref):
    parts = [(ref, seen(off_ref[2 + i], lim_ref, ref)) for i, ref in enumerate((side_ref, both_ref))]
    o_ref[...] = (near_ref[...] + attend_pair(q_ref[...], parts, slice(None))).astype(BF16)


def finish_kernel(t_ref, gate_ref, x_ref, w_ref, o_ref):
    sides = [jnp.sum(t_ref[h].astype(F32), axis=0) for h in range(t_ref.shape[0])]
    total = jnp.concatenate(sides, axis=1)
    mixed = (center(total) * gate_ref[...]).astype(BF16)
    o_ref[...] = (x_ref[...].astype(F32) + jnp.dot(mixed, w_ref[...], preferred_element_type=F32)).astype(BF16)


def sds(shape, dtype=BF16):
    return jax.ShapeDtypeStruct(shape, dtype)


def layer(cand_x, hist_keys, hist_values, key_scale, hist_len, cand_limit, ln_gain, w_qu, w_out):
    own, width = cand_x.shape
    n = hist_keys.shape[0]
    pairs = lax.axis_size("pair")
    pair = lax.axis_index("pair")
    side = lax.axis_index("side")
    z = lax.axis_index("z")
    part = width // 4
    rows = 4 * pairs * own

    def exchange(t):
        return lax.all_to_all(t.reshape(4 * pairs, own, part), ("z", "side", "pair"), 0, 0, tiled=True)

    gain = ln_gain.reshape(1, width)
    q = pl.pallas_call(
        project_kernel, out_shape=sds((4, pairs, own, part)), in_specs=[HB] * 3, out_specs=VM,
        scratch_shapes=[
            pltpu.VMEM((own, width), BF16), pltpu.VMEM((1, width), F32), pltpu.VMEM((width, width), BF16),
            pltpu.SemaphoreType.DMA((3,)),
        ],
        compiler_params=PARAMS, name="project",
    )(*(pltpu.with_memory_space_constraint(v, pltpu.HBM) for v in (cand_x, gain, w_qu)))
    gate = pl.pallas_call(
        gate_kernel, out_shape=sds((own, width), F32), in_specs=[VM] * 3, out_specs=VM,
        compiler_params=PARAMS, name="gate",
    )(cand_x, gain, w_qu)
    every_q = exchange(q).reshape(rows, part)
    own_kv, to_side, to_z, to_both = pl.pallas_call(
        pack_kernel, out_shape=(sds((2 * n, part)),) * 4,
        in_specs=[SM] + [VM] * 3, out_specs=(VM,) * 4, compiler_params=PARAMS, name="pack",
    )((z * 2 + side).astype(jnp.int32).reshape(1), hist_keys, hist_values, key_scale)
    z_kv = lax.ppermute(to_z, "z", [(0, 1), (1, 0)])
    both_kv = lax.ppermute(to_both, ("side", "z"), [(i, 3 - i) for i in range(4)])
    side_kv = lax.ppermute(to_side, "side", [(0, 1), (1, 0)])

    limits = jnp.minimum(cand_limit, hist_len[0]).reshape(pairs, 2, 2, own)
    limits = jnp.transpose(limits, (2, 1, 0, 3)).reshape(rows, 1)
    offsets = jnp.stack(
        [((pair * 2 + s) * 2 + t) * n for s, t in ((side, z), (1 - side, 1 - z), (side, 1 - z), (1 - side, z))]
    ).astype(jnp.int32)

    total = pl.pallas_call(
        near_kernel, out_shape=sds((rows, part), F32), in_specs=[SM] + [VM] * 4, out_specs=VM,
        compiler_params=PARAMS, name="near",
    )(offsets, every_q, own_kv, both_kv, limits)
    total = pl.pallas_call(
        far_kernel, out_shape=sds((rows, part)), in_specs=[SM] + [VM] * 5, out_specs=VM,
        compiler_params=PARAMS, name="far",
    )(offsets, every_q, z_kv, side_kv, limits, total)
    totals = exchange(total).reshape(4, pairs, own, part)
    return pl.pallas_call(
        finish_kernel, out_shape=sds((own, width)), in_specs=[VM] * 4, out_specs=VM,
        compiler_params=PARAMS, name="finish",
    )(totals, gate, cand_x, w_out)


def solution(mesh):
    users, hist = mesh.devices.shape
    grid = Mesh(mesh.devices.reshape(users, hist // 4, 2, 2), ("users", "pair", "side", "z"))
    both = ("users", "pair", "side", "z")
    in_specs = (P(both, None), P(both, None), P(both, None), P(both), P("users"), P("users"), P(), P(), P())
    return jax.shard_map(layer, mesh=grid, in_specs=in_specs, out_specs=P(both, None), check_vma=False)
```

```python
import jax
import jax.numpy as jnp
from jax import lax
from jax.experimental import pallas as pl
from jax.experimental.pallas import tpu as pltpu
from jax.sharding import Mesh, PartitionSpec as P


F32 = jnp.float32
BF16 = jnp.bfloat16
VM = pl.BlockSpec(memory_space=pltpu.VMEM)
HB = pl.BlockSpec(memory_space=pltpu.HBM)
SM = pl.BlockSpec(memory_space=pltpu.SMEM)
PARAMS = pltpu.CompilerParams(vmem_limit_bytes=40 * 1024 * 1024)


def center(v):
    mean = jnp.mean(v, axis=-1, keepdims=True)
    var = jnp.mean((v - mean) ** 2, axis=-1, keepdims=True)
    return (v - mean) / jnp.sqrt(var + 1e-5)


def front_kernel(
    part_ref, x_hbm, gain_hbm, w_hbm, k_hbm, v_hbm, s_hbm, q_hbm, own_ref, side_ref, z_ref, both_ref,
    x_ref, gain_ref, w_ref, k_ref, v_ref, s_ref, q_ref, sems, q_sems,
):
    width = w_ref.shape[1]
    sources = (x_hbm, gain_hbm, w_hbm.at[:, pl.ds(0, width)], k_hbm, s_hbm, v_hbm)
    targets = (x_ref, gain_ref, w_ref, k_ref, s_ref, v_ref)
    loads = [pltpu.make_async_copy(a, b, sems.at[i]) for i, (a, b) in enumerate(zip(sources, targets))]
    for load in loads:
        load.start()
    loads[0].wait()
    loads[1].wait()
    normed = (center(x_ref[...].astype(F32)) * gain_ref[...]).astype(BF16)
    loads[2].wait()
    p = jnp.dot(normed, w_ref[...], preferred_element_type=F32)
    q = (p / (1.0 + jnp.exp(-p))).astype(BF16)
    parts, _, part = q_ref.shape
    for h in range(parts):
        q_ref[h] = q[:, h * part:(h + 1) * part]
    stores = [pltpu.make_async_copy(q_ref, q_hbm.at[:, i], q_sems.at[i]) for i in range(q_hbm.shape[1])]
    for store in stores:
        store.start()
    for load in loads[3:]:
        load.wait()
    pack(part_ref, k_ref, v_ref, s_ref, own_ref, side_ref, z_ref, both_ref)
    for store in stores:
        store.wait()


def gate_kernel(x_ref, gain_ref, w_ref, gate_ref):
    width = x_ref.shape[1]
    normed = (center(x_ref[...].astype(F32)) * gain_ref[...]).astype(BF16)
    p = jnp.dot(normed, w_ref[:, width:], preferred_element_type=F32)
    gate_ref[...] = p / (1.0 + jnp.exp(-p))


def pack(part_ref, k_ref, v_ref, s_ref, *outs):
    rows, width = k_ref.shape
    part = width // len(outs)
    col = jnp.broadcast_to(s_ref[...].astype(F32).reshape(1, rows) * (1.0 / 16.0), (8, rows)).T[:, :1]
    k = (k_ref[...].astype(F32) * col).astype(BF16)
    for h in range(len(outs)):

        @pl.when(part_ref[0] == h)
        def _():
            for flip, out in enumerate(outs):
                cs = slice((h ^ flip) * part, ((h ^ flip) + 1) * part)
                out[:rows] = k[:, cs]
                out[rows:] = v_ref[:, cs]


def attend_pair(q, parts, cs):
    low = lax.broadcasted_iota(jnp.int32, (1, 128), 1) < 64
    weights = []
    values = []
    for kv_ref, mask in parts:
        n = kv_ref.shape[0] // 2
        k = kv_ref[:n, cs]
        v = kv_ref[n:, cs]
        for sel in (low, jnp.logical_not(low)):
            head = jnp.where(sel, q, jnp.zeros_like(q))
            u = lax.dot_general(head, k, (((1,), (1,)), ((), ())), preferred_element_type=F32)
            weights.append((u * (1.0 + jnp.tanh(u))).astype(BF16) * mask)
            values.append(jnp.where(sel, v, jnp.zeros_like(v)))
    return jnp.dot(jnp.concatenate(weights, 1), jnp.concatenate(values, 0), preferred_element_type=F32)


def seen(off, lim_ref, kv_ref):
    pos = lax.broadcasted_iota(jnp.int32, (lim_ref.shape[0], kv_ref.shape[0] // 2), 1) + off
    return jnp.where(pos < lim_ref[...], 1.0, 0.0).astype(BF16)


def near_kernel(off_ref, q_ref, own_ref, side_ref, lim_ref, o_ref):
    parts = [(ref, seen(off_ref[i], lim_ref, ref)) for i, ref in enumerate((own_ref, side_ref))]
    o_ref[...] = attend_pair(q_ref[...], parts, slice(None))


def far_kernel(off_ref, q_ref, side_ref, both_ref, lim_ref, near_ref, o_ref):
    parts = [(ref, seen(off_ref[2 + i], lim_ref, ref)) for i, ref in enumerate((side_ref, both_ref))]
    o_ref[...] = (near_ref[...] + attend_pair(q_ref[...], parts, slice(None))).astype(BF16)


def finish_kernel(t_ref, gate_ref, x_ref, w_ref, o_ref):
    sides = [jnp.sum(t_ref[h].astype(F32), axis=0) for h in range(t_ref.shape[0])]
    total = jnp.concatenate(sides, axis=1)
    mixed = (center(total) * gate_ref[...]).astype(BF16)
    o_ref[...] = (x_ref[...].astype(F32) + jnp.dot(mixed, w_ref[...], preferred_element_type=F32)).astype(BF16)


def sds(shape, dtype=BF16):
    return jax.ShapeDtypeStruct(shape, dtype)


def layer(cand_x, hist_keys, hist_values, key_scale, hist_len, cand_limit, ln_gain, w_qu, w_out):
    own, width = cand_x.shape
    n = hist_keys.shape[0]
    pairs = lax.axis_size("pair")
    pair = lax.axis_index("pair")
    side = lax.axis_index("side")
    z = lax.axis_index("z")
    part = width // 4
    rows = 4 * pairs * own

    def exchange(t):
        return lax.all_to_all(t.reshape(4 * pairs, own, part), ("z", "side", "pair"), 0, 0, tiled=True)

    gain = ln_gain.reshape(1, width)
    hbm = [pltpu.with_memory_space_constraint(v, pltpu.HBM) for v in (cand_x, gain, w_qu, hist_keys, hist_values, key_scale)]
    q, own_kv, to_side, to_z, to_both = pl.pallas_call(
        front_kernel, out_shape=(sds((4, pairs, own, part)),) + (sds((2 * n, part)),) * 4,
        in_specs=[SM] + [HB] * 6, out_specs=(HB,) + (VM,) * 4,
        scratch_shapes=[
            pltpu.VMEM((own, width), BF16), pltpu.VMEM((1, width), F32), pltpu.VMEM((width, width), BF16),
            pltpu.VMEM((n, width), BF16), pltpu.VMEM((n, width), BF16), pltpu.VMEM((n,), BF16),
            pltpu.VMEM((4, own, part), BF16),
            pltpu.SemaphoreType.DMA((6,)), pltpu.SemaphoreType.DMA((pairs,)),
        ],
        compiler_params=PARAMS, name="front",
    )((z * 2 + side).astype(jnp.int32).reshape(1), *hbm)
    gate = pl.pallas_call(
        gate_kernel, out_shape=sds((own, width), F32), in_specs=[VM] * 3, out_specs=VM,
        compiler_params=PARAMS, name="gate",
    )(cand_x, gain, w_qu)
    every_q = exchange(q).reshape(rows, part)
    z_kv = lax.ppermute(to_z, "z", [(0, 1), (1, 0)])
    both_kv = lax.ppermute(to_both, ("side", "z"), [(i, 3 - i) for i in range(4)])
    side_kv = lax.ppermute(to_side, "side", [(0, 1), (1, 0)])

    limits = jnp.minimum(cand_limit, hist_len[0]).reshape(pairs, 2, 2, own)
    limits = jnp.transpose(limits, (2, 1, 0, 3)).reshape(rows, 1)
    offsets = jnp.stack(
        [((pair * 2 + s) * 2 + t) * n for s, t in ((side, z), (1 - side, 1 - z), (side, 1 - z), (1 - side, z))]
    ).astype(jnp.int32)

    total = pl.pallas_call(
        near_kernel, out_shape=sds((rows, part), F32), in_specs=[SM] + [VM] * 4, out_specs=VM,
        compiler_params=PARAMS, name="near",
    )(offsets, every_q, own_kv, both_kv, limits)
    total = pl.pallas_call(
        far_kernel, out_shape=sds((rows, part)), in_specs=[SM] + [VM] * 5, out_specs=VM,
        compiler_params=PARAMS, name="far",
    )(offsets, every_q, z_kv, side_kv, limits, total)
    totals = exchange(total).reshape(4, pairs, own, part)
    return pl.pallas_call(
        finish_kernel, out_shape=sds((own, width)), in_specs=[VM] * 4, out_specs=VM,
        compiler_params=PARAMS, name="finish",
    )(totals, gate, cand_x, w_out)


def solution(mesh):
    users, hist = mesh.devices.shape
    grid = Mesh(mesh.devices.reshape(users, hist // 4, 2, 2), ("users", "pair", "side", "z"))
    both = ("users", "pair", "side", "z")
    in_specs = (P(both, None), P(both, None), P(both, None), P(both), P("users"), P("users"), P(), P(), P())
    return jax.shard_map(layer, mesh=grid, in_specs=in_specs, out_specs=P(both, None), check_vma=False)
```
